512 devices in a mesh: row: 16 (over y, core), col: 32 (over z, x).
Axes of the slice: x: 4, y: 8, z: 8, core: 2. Of those that a mesh axis runs over, the one named last changes fastest.
Arguments:
- offsets: float32 [3, 131072], P(None, ('row', 'col')), may hold values from 0 to 11
- cells: int32 [3, 1024], replicated, may hold values from 0 to 15, as said below
- types: int32 [131072], P(('row', 'col')), may hold values from 0 to 3, as said below
- mask: int32 [16, 64, 16, 64], P(None, 'col', 'row'), may hold values from 0 to 1, as said below
- chi_table: float32 [4], replicated, may hold values from 2 to 10.1
- eta_table: float32 [4], replicated, may hold values from 13 to 18
- gamma_table: float32 [4], replicated, may hold values from 0.4 to 0.8
Outputs:
- charges: float32 [131072], P(('row', 'col'))
The draws below stay inside these ranges and needn't reach their ends.
Inputs may be any that keep to these rules, and one draw needn't show every extreme that they name: The cells of the blocks are a permutation of all 16 x 16 x 4 cells: each cell holds exactly one block. The mask marks a pair of blocks exactly when their cells are equal or adjacent on the periodic grid in every dimension; it is symmetric and each block is marked with exactly 27 blocks, itself included. `types`: types 2 and 3 grow more common along the atoms, from none in the first 256 atoms to nearly all in the last.
All inputs are finite; a program needn't handle non-finite values.
Results may differ from the reference program's by a relative error of at most 0.0003.
Values sent between devices are 32-bit elements; how exact they have to be, the bound alone decides.
A program may use at most 64 MiB of HBM per device.

```python
import math
import jax
import jax.numpy as jnp
from jax import lax

BLOCK = 128
BPD = 2
NTYPES = 4
NEIGHBORS = 27
GRID_Z = 4
ITERS = 3
RB = 64
NB = 1024
ATOMS = 131072
SPAN = 256
GRID_X = 16
GRID_Y = 16
N_ROW = 16


def block_cells(key):
    order = jax.random.permutation(jax.random.fold_in(key, 11), NB).astype(jnp.int32)
    first = order // (GRID_Y * GRID_Z)
    second = order // GRID_Z % GRID_Y
    third = order % GRID_Z
    return jnp.stack([first, second, third], axis=0)


def draw_cells(key, part):
    return block_cells(key)


def draw_mask(key, part):
    placed = block_cells(key)
    grid = jnp.array([GRID_X, GRID_Y, GRID_Z], jnp.int32)[:, None, None]
    diff = placed[:, :, None] - placed[:, None, :]
    wrapped = (diff + grid // 2) % grid - grid // 2
    near = jnp.all(jnp.abs(wrapped) <= 1, axis=0).astype(jnp.int32)
    return near.reshape(N_ROW, RB, N_ROW, RB)


def draw_types(key, part):
    spans = NB // BPD
    owner = jnp.arange(ATOMS, dtype=jnp.int32) // SPAN
    level = jax.random.randint(jax.random.fold_in(key, 21), (ATOMS,), 0, spans)
    within = jax.random.randint(jax.random.fold_in(key, 22), (ATOMS,), 0, 2)
    return (2 * (level < owner).astype(jnp.int32) + within).astype(jnp.int32)


def draw_chi_table(key, part):
    base = 2.0 + 2.2 * jnp.arange(NTYPES, dtype=jnp.float32)
    jitter = jax.random.uniform(jax.random.fold_in(key, 31), (NTYPES,), jnp.float32, 0.0, 1.5)
    return (base + jitter).astype(jnp.float32)


def block_scale(stream_key, dims, split, low, largest):
    loudness = 1.0
    for axis_at, parts in split:
        draws = jax.random.uniform(jax.random.fold_in(jax.random.fold_in(stream_key, 6), axis_at), (parts,), jnp.float32, low / len(split), largest / len(split))
        loudness = loudness * jnp.repeat(jnp.exp(draws), dims[axis_at] // parts).reshape((-1,) + (1,) * (len(dims) - 1 - axis_at))
    return loudness


def setup_inputs(seed: int = 0) -> dict:
    key_list = jax.random.split(jax.random.key(seed), 8)
    offsets = jnp.clip(11.0 * jax.random.uniform(key_list[0], (3, ATOMS), jnp.float32) ** block_scale(key_list[0], (3, ATOMS), ((1, 512),), -0.2, 0.2), 0.0, 11.0)
    cells = draw_cells(jax.random.fold_in(key_list[7], 71), 0)
    types = draw_types(jax.random.fold_in(key_list[7], 71), 0)
    mask = draw_mask(jax.random.fold_in(key_list[7], 71), 0)
    chi_table = draw_chi_table(jax.random.fold_in(key_list[7], 71), 0)
    eta_table = jnp.clip(jax.random.uniform(key_list[5], (NTYPES,), jnp.float32, 13.0, 18.0), 13.0, 18.0)
    gamma_table = jnp.clip(jnp.exp(jax.random.uniform(key_list[6], (NTYPES,), jnp.float32, math.log(0.4), math.log(0.8))), 0.4, 0.8)
    return dict(offsets=offsets, cells=cells, types=types, mask=mask, chi_table=chi_table, eta_table=eta_table, gamma_table=gamma_table)


coulomb = 14.4
cutoff = 10.0
cell_side = 11.0
ref_group = 64

def taper(dist):
    xval = dist / cutoff
    poly = 1.0 + xval ** 4 * (-35.0 + xval * (84.0 + xval * (-70.0 + 20.0 * xval)))
    return jnp.where(xval < 1.0, poly, 0.0)

def coupling(tgt, src, tgt_cell, src_cell, same, grid):
    half = grid[:, None] // 2
    shift = ((src_cell - tgt_cell + half) % grid[:, None] - half).astype(jnp.float32) * cell_side
    radius_sq = jnp.zeros((tgt.shape[1], tgt.shape[2], src.shape[2]), jnp.float32)
    for comp in range(3):
        delta = shift[comp][:, None, None] + src[comp][:, None, :] - tgt[comp][:, :, None]
        radius_sq = radius_sq + delta * delta
    dist = jnp.sqrt(radius_sq)
    paired = tgt[3][:, :, None] * src[3][:, None, :]
    shield = 1.0 / (paired * jnp.sqrt(paired))
    kern = coulomb * taper(dist) / jnp.cbrt(radius_sq * dist + shield)
    width = tgt.shape[2]
    diag = jnp.arange(width)[:, None] == jnp.arange(width)[None, :]
    return jnp.where(same[:, None, None] & diag[None], 0.0, kern)

def pick(kinds, table):
    return lax.optimization_barrier(jnp.sum(jnp.where(kinds, table[:, None], 0.0), axis=0))

def reference(offsets, cells, types, mask, chi_table, eta_table, gamma_table):
    nblocks = cells.shape[1]
    kinds = jnp.arange(chi_table.shape[0])[:, None] == types[None, :]
    chi = pick(kinds, chi_table)
    eta = pick(kinds, eta_table)
    gamma = pick(kinds, gamma_table)
    geo = jnp.concatenate([offsets, gamma[None]], axis=0).reshape(4, nblocks, BLOCK)
    grid = jnp.array([GRID_X, GRID_Y, GRID_Z], jnp.int32)
    flat = mask.reshape(nblocks * nblocks)
    marked = jnp.sum(flat)
    groups = (nblocks * NEIGHBORS + ref_group - 1) // ref_group
    slots = jnp.nonzero(flat, size=groups * ref_group, fill_value=0)[0].astype(jnp.int32)
    block_ids = jnp.arange(nblocks, dtype=jnp.int32)

    def matvec(vec):
        spread = vec.reshape(2, nblocks, BLOCK)

        def turn(acc, step):
            picked = lax.dynamic_slice_in_dim(slots, step * ref_group, ref_group)
            live = step * ref_group + jnp.arange(ref_group) < marked
            tgt_blk = picked // nblocks
            src_blk = picked % nblocks
            kern = coupling(geo[:, tgt_blk], geo[:, src_blk], cells[:, tgt_blk], cells[:, src_blk], block_ids[tgt_blk] == block_ids[src_blk], grid)
            kern = jnp.where(live[:, None, None], kern, 0.0)
            contrib = jnp.einsum('gij,kgj->kgi', kern, spread[:, src_blk], precision=lax.Precision.HIGHEST)
            return (acc.at[:, tgt_blk].add(contrib), None)
        acc, _ = lax.scan(turn, jnp.zeros((2, nblocks, BLOCK), jnp.float32), jnp.arange(groups, dtype=jnp.int32))
        return acc.reshape(2, nblocks * BLOCK) + eta[None] * vec
    rhs = jnp.stack([-chi, -jnp.ones_like(chi)], axis=0)
    solution = jnp.zeros_like(rhs)
    residual = rhs
    direction = rhs
    norm_now = lax.optimization_barrier(jnp.sum(residual * residual, axis=1))
    for step in range(ITERS):
        image = matvec(direction)
        alpha = norm_now / lax.optimization_barrier(jnp.sum(direction * image, axis=1))
        solution = solution + alpha[:, None] * direction
        residual = residual - alpha[:, None] * image
        norm_next = lax.optimization_barrier(jnp.sum(residual * residual, axis=1))
        direction = residual + (norm_next / norm_now)[:, None] * direction
        norm_now = norm_next
    totals = lax.optimization_barrier(jnp.sum(solution, axis=1))
    return solution[0] - totals[0] / totals[1] * solution[1]
```

```python
import jax
import jax.numpy as jnp
from jax import lax
from jax.experimental import pallas as pl
from jax.experimental.pallas import tpu as pltpu
from jax.sharding import Mesh
from jax.sharding import PartitionSpec as P

LANES = 128
NX, NY, NZ, NQ = 4, 8, 8, 16
OWN = 17
PAIRS = 27
SLOTS = 36
MOMENTS = 10
SHIFTS = (200.0, 20.0)
F32 = jnp.float32
AXES = ("y", "c", "z", "x")
HIGH = lax.Precision.HIGHEST
HALO = [(a, b, d) for a in (-1, 0, 1) for b in (-1, 0, 1) for d in (-1, 0, 1) if (a, b, d) != (0, 0, 0)]


def far_first(n):
    return sorted(range(1, n), key=lambda k: -min(k, n - k))


def choose(kind, table):
    low = jnp.where(kind < 0.5, table[0], table[1])
    high = jnp.where(kind < 2.5, table[2], table[3])
    return jnp.where(kind < 1.5, low, high)


class Exchange:
    def __init__(self, peers, send, recv):
        self.peers, self.send, self.recv = peers, send, recv
        self.copies = []

    def start(self, src, dst):
        self.copies = []
        for k, peer in self.peers:
            copy = pltpu.make_async_remote_copy(
                src_ref=src(k),
                dst_ref=dst(k),
                send_sem=self.send.at[k],
                recv_sem=self.recv.at[k],
                device_id=peer,
                device_id_type=pl.DeviceIdType.MESH,
            )
            copy.start()
            self.copies.append(copy)

    def wait(self):
        for copy in self.copies:
            copy.wait_recv()

    def finish(self):
        for copy in self.copies:
            copy.wait_send()


def kernel(
    idx, chi_t, eta_t, gam_t, off, typ, out,
    gat, sel, rcv, hal, feat, tgt, hbuf, hv0, hv1, hv2,
    rgat, rsel, rrcv, own0, az, ax, aq, msgs,
    zs, zr, xs, xr, qs, qr, hs, hr, h1s, h1r, h2s, h2r,
    rzs, rzr, rxs, rxr, rqs, rqr, dzs, dzr, dxs, dxr, dqs, dqr,
):
    my = lax.axis_index("y")
    mc = lax.axis_index("c")
    mz = lax.axis_index("z")
    mx = lax.axis_index("x")
    mq = my * 2 + mc
    gx = mz * 2 + mc
    zpeers = [(k, {"z": lax.rem(mz + k, NZ)}) for k in far_first(NZ)]
    xpeers = [(k, {"x": lax.rem(mx + k, NX)}) for k in far_first(NX)]
    qpeers = []
    for k in sorted(range(1, NQ), key=lambda k: -min(k, NQ - k)):
        q = lax.rem(mq + k, NQ)
        qpeers.append((k, {"y": q // 2, "c": lax.rem(q, 2)}))
    hpeers = []
    for k, (ex, ez, ey) in enumerate(HALO):
        g = lax.rem(gx + ex + 16, 16)
        hpeers.append((k, {
            "z": g // 2, "c": lax.rem(g, 2),
            "x": lax.rem(mx + ez + NX, NX), "y": lax.rem(my + ey + NY, NY),
        }))

    barrier = pltpu.get_barrier_semaphore()
    everyone = zpeers + xpeers + qpeers + hpeers
    for _, peer in everyone:
        pl.semaphore_signal(barrier, inc=1, device_id=peer, device_id_type=pl.DeviceIdType.MESH)

    for b in range(2):
        lanes = pl.ds(b * LANES, LANES)
        kind = typ[b : b + 1, :].astype(F32)
        for comp in range(3):
            gat[mx, mz, b, comp : comp + 1, :] = off[comp : comp + 1, lanes]
        gat[mx, mz, b, 3:4, :] = kind
        own0[b, 0:1, :] = -choose(kind, chi_t)
        own0[b, 1:2, :] = jnp.full((1, LANES), -1.0, F32)
    pl.semaphore_wait(barrier, len(everyone))

    def half(k):
        return (0, 2) if HALO[k][2] == 0 else ((1, 1) if HALO[k][2] == 1 else (0, 1))

    def halo_src(ref):
        return lambda k: ref.at[pl.ds(OWN + half(k)[0], half(k)[1])]

    def halo_dst(ref):
        def at(k):
            ex, ez, ey = HALO[k]
            first, n = half(k)
            slot = ((1 - ex) * 3 + (1 - ez)) * 4 + first + 1 - 2 * ey
            return ref.at[pl.ds(slot, n)]
        return at

    zg = Exchange(zpeers, zs, zr)
    zg.start(lambda k: gat.at[mx, mz], lambda k: gat.at[mx, mz])
    zg.wait()
    xg = Exchange(xpeers, xs, xr)
    xg.start(lambda k: gat.at[mx], lambda k: gat.at[mx])
    xg.wait()

    def to_q(q, base, source, chosen):
        for s in range(2):
            i = idx[base + q * 2 + s]
            chosen[q, s] = source[i // 16, lax.rem(i, 16) // 2, lax.rem(i, 2)]

    def pick_all(base, source, chosen, received):
        def one(q, carry):
            to_q(q, base, source, chosen)
            return carry
        lax.fori_loop(0, NQ, one, 0, unroll=True)
        for s in range(2):
            i = idx[base + mq * 2 + s]
            received[mq, s] = source[i // 16, lax.rem(i, 16) // 2, lax.rem(i, 2)]

    pick_all(0, gat, sel, rcv)
    qg = Exchange(qpeers, qs, qr)
    qg.start(lambda k: sel.at[lax.rem(mq + k, NQ)], lambda k: rcv.at[mq])
    qg.wait()
    for s in range(2):
        hal[OWN + s] = rcv[idx[64 + s], s]
    hg = Exchange(hpeers, hs, hr)
    hg.start(halo_src(hal), halo_dst(hal))

    comp = lax.broadcasted_iota(jnp.int32, (4, LANES), 0)

    def features(slot):
        raw = hal[slot]
        sx = (slot // 12 - 1) * 11
        sz = (lax.rem(slot, 12) // 4 - 1) * 11
        sy = (lax.rem(slot, 4) - 1) * 11
        shift = jnp.where(comp == 0, sx, jnp.where(comp == 1, sy, sz)).astype(F32)
        kind = hal[slot, 3:4, :]
        gam = choose(kind, gam_t)
        shield = (lax.rsqrt(gam) / gam) * (0.001 ** 0.5)
        feat[slot] = jnp.where(comp == 3, jnp.broadcast_to(shield, (4, LANES)), (raw + shift) * 0.1)
        hv0[slot, 0:1, :] = -choose(kind, chi_t)
        hv0[slot, 1:2, :] = jnp.full((1, LANES), -1.0, F32)

    for t in range(2):
        features(OWN + t)
        for c in range(4):
            tgt[t, c] = jnp.broadcast_to(feat[OWN + t, c : c + 1, :], (LANES, LANES)).T

    hg.wait()

    def all_features(slot, carry):
        features(slot)
        return carry
    lax.fori_loop(0, SLOTS, all_features, 0)

    for t in range(2):
        def one_pair(n, carry):
            slot = (n // 3) * 4 + lax.rem(n, 3) + t
            src = [feat[slot, c : c + 1, :] for c in range(4)]
            for j in range(16):
                rows = pl.ds(j * 8, 8)
                dx = src[0] - tgt[t, 0, rows, :]
                dy = src[1] - tgt[t, 1, rows, :]
                dz = src[2] - tgt[t, 2, rows, :]
                r2 = jnp.maximum(dx * dx + dy * dy + dz * dz, 1e-30)
                r = r2 * lax.rsqrt(r2)
                cube = r2 * r + src[3] * tgt[t, 3, rows, :]
                inv = jnp.exp2(jnp.log2(cube) * (-1.0 / 3.0))
                u = jnp.maximum(1.0 - r, 0.0)
                u = u * u
                poly = ((28.8 * r + 14.4) * r + 5.76) * r + 1.44
                hbuf[t, n, rows, :] = (u * u) * poly * inv
            return carry
        lax.fori_loop(0, PAIRS, one_pair, 0)
        eta = choose(hal[OWN + t, 3:4, :], eta_t)
        diag = lax.broadcasted_iota(jnp.int32, (LANES, LANES), 0) == lax.broadcasted_iota(jnp.int32, (LANES, LANES), 1)
        hbuf[t, 13] = jnp.where(diag, eta, hbuf[t, 13])

    ones = jnp.ones((8, LANES), F32)
    rhs_row = lax.broadcasted_iota(jnp.int32, (2, LANES), 0)

    def matvec(vec):
        res = []
        for t in range(2):
            def near(n, carry):
                acc_s, acc_t = carry
                for d in range(3):
                    h = hbuf[t, n * 3 + d]
                    v = vec[n * 4 + d + t]
                    acc_s = acc_s + h * v[0:1, :]
                    acc_t = acc_t + h * v[1:2, :]
                return acc_s, acc_t
            zero = jnp.zeros((LANES, LANES), F32)
            acc_s, acc_t = lax.fori_loop(0, 9, near, (zero, zero))
            dims = (((1,), (1,)), ((), ()))
            sum_s = lax.dot_general(ones, acc_s, dims, precision=HIGH, preferred_element_type=F32)
            sum_t = lax.dot_general(ones, acc_t, dims, precision=HIGH, preferred_element_type=F32)
            res.append(jnp.where(rhs_row == 0, sum_s[0:2], sum_t[0:2]))
        return res

    v1 = matvec(hv0)
    for t in range(2):
        hv1[OWN + t] = v1[t] - SHIFTS[0] * hv0[OWN + t]
    g1 = Exchange(hpeers, h1s, h1r)
    g1.start(halo_src(hv1), halo_dst(hv1))
    g1.wait()
    v2 = matvec(hv1)
    for t in range(2):
        hv2[OWN + t] = v2[t] - SHIFTS[1] * hv1[OWN + t]
    g2 = Exchange(hpeers, h2s, h2r)
    g2.start(halo_src(hv2), halo_dst(hv2))
    for t in range(2):
        rgat[mx, mz, t, 0:2, :] = hv1[OWN + t]
        rgat[mx, mz, t, 2:4, :] = hv2[OWN + t]
    rz = Exchange(zpeers, rzs, rzr)
    rz.start(lambda k: rgat.at[mx, mz], lambda k: rgat.at[mx, mz])
    g2.wait()
    v3 = matvec(hv2)

    lane = lax.broadcasted_iota(jnp.int32, (2, LANES), 1)
    v = [[hv0[OWN + t] for t in range(2)], [hv1[OWN + t] for t in range(2)], [hv2[OWN + t] for t in range(2)], v3]
    terms = [v[a][0] * v[b][0] + v[a][1] * v[b][1] for a, b in ((0, 0), (0, 1), (0, 2), (1, 1), (1, 2), (2, 2), (2, 3))]
    terms += [v[a][0] + v[a][1] for a in range(3)]
    msg = jnp.zeros((2, LANES), F32)
    for k, term in enumerate(terms):
        msg = jnp.where(lane == k, jnp.sum(term, axis=1, keepdims=True), msg)
    msgs[0] = msg
    az[mz] = msg
    dz_ = Exchange(zpeers, dzs, dzr)
    dz_.start(lambda k: msgs.at[0], lambda k: az.at[mz])
    rz.wait()
    rx = Exchange(xpeers, rxs, rxr)
    rx.start(lambda k: rgat.at[mx], lambda k: rgat.at[mx])
    dz_.wait()
    msg = az[0]
    for k in range(1, NZ):
        msg = msg + az[k]
    msgs[1] = msg
    ax[mx] = msg
    dx_ = Exchange(xpeers, dxs, dxr)
    dx_.start(lambda k: msgs.at[1], lambda k: ax.at[mx])
    rx.wait()
    pick_all(32 + 34, rgat, rsel, rrcv)
    rq = Exchange(qpeers, rqs, rqr)
    rq.start(lambda k: rsel.at[lax.rem(mq + k, NQ)], lambda k: rrcv.at[mq])
    dx_.wait()
    msg = ax[0]
    for k in range(1, NX):
        msg = msg + ax[k]
    msgs[2] = msg
    aq[mq] = msg
    dq_ = Exchange(qpeers, dqs, dqr)
    dq_.start(lambda k: msgs.at[2], lambda k: aq.at[mq])
    rq.wait()
    back = [rrcv[idx[130 + s], s] for s in range(2)]
    dq_.wait()
    msg = aq[0]
    for k in range(1, NQ):
        msg = msg + aq[k]

    m = [jnp.broadcast_to(msg[:, k : k + 1], (2, LANES)) for k in range(MOMENTS)]
    gram = {(0, 0): m[0], (0, 1): m[1], (0, 2): m[2], (1, 1): m[3], (1, 2): m[4], (2, 2): m[5]}
    sums = m[7:]

    def dot(i, j):
        return gram[min(i, j), max(i, j)]

    def image_dot(i, j):
        i, j = min(i, j), max(i, j)
        return m[6] if i == 2 else dot(i + 1, j) + SHIFTS[i] * dot(i, j)

    def quadratic(a, form):
        total = None
        for i, ai in enumerate(a):
            for j in range(i, len(a)):
                term = ai * a[j] * form(i, j)
                term = term if i == j else term + term
                total = term if total is None else total + term
        return total

    def image(a):
        res = [None] * (len(a) + 1)
        for i, ai in enumerate(a):
            res[i + 1] = ai
            res[i] = SHIFTS[i] * ai if res[i] is None else res[i] + SHIFTS[i] * ai
        return res

    def plus(a, scale, b):
        res = []
        for i in range(max(len(a), len(b))):
            ai = a[i] if i < len(a) else None
            bi = b[i] if i < len(b) else None
            if bi is None:
                res.append(ai)
            elif ai is None:
                res.append(scale * bi)
            else:
                res.append(ai + scale * bi)
        return res

    one = jnp.ones((2, LANES), F32)
    x, r, p = [], [one], [one]
    rr = m[0]
    for step in range(3):
        alpha = rr / quadratic(p, image_dot)
        x = plus(x, alpha, p)
        if step < 2:
            r = plus(r, -alpha, image(p))
            new = quadratic(r, dot)
            p = plus(r, new / rr, p)
            rr = new
    total = x[0] * sums[0] + x[1] * sums[1] + x[2] * sums[2]
    ratio = total[0:1] / total[1:2]
    for s in range(2):
        b = back[s]
        part = x[0] * own0[s] + x[1] * b[0:2] + x[2] * b[2:4]
        out[s : s + 1, :] = part[0:1] - ratio * part[1:2]

    for e in (zg, xg, qg, hg, g1, g2, rz, rx, rq, dz_, dx_, dq_):
        e.finish()


def place(cell):
    return cell[2] * 8 + cell[0] // 2, cell[1] % 2, (cell[1] // 2) * 2 + cell[0] % 2


def per_device(offsets, cells, types, mask, chi_table, eta_table, gamma_table):
    my, mc = lax.axis_index("y"), lax.axis_index("c")
    mz, mx = lax.axis_index("z"), lax.axis_index("x")
    mq = my * 2 + mc
    col = mz * 4 + mx
    nb = cells.shape[1]
    key = (cells[0] * 16 + cells[1]) * 4 + cells[2]
    q = jnp.arange(32, dtype=jnp.int32) // 2
    s = jnp.arange(32, dtype=jnp.int32) % 2

    def target(q, s):
        return ((2 * mz + q % 2) * 16 + 2 * (q // 2) + s) * 4 + mx

    two = jnp.arange(2, dtype=jnp.int32)
    wanted = jnp.concatenate([target(q, s), target(mq, two)])
    ids = jnp.arange(nb, dtype=jnp.int32)
    block = jnp.sum(jnp.where(key[None, :] == wanted[:, None], ids[None, :], 0), axis=1).astype(jnp.int32)
    local = block % 64
    at = local // 2
    fwd = ((at % 4) * 8 + at // 4) * 2 + local % 2
    fwd_owner = block // 64
    mine = jnp.concatenate([q * 64 + col * 2 + s, mq * 64 + col * 2 + two])
    cell = jnp.take(cells, mine, axis=1)
    spot, slot, holder = place(cell)
    rev = spot * 2 + slot
    idx = jnp.concatenate([
        fwd[:32], jnp.zeros((32,), jnp.int32), fwd_owner[32:], rev[:32], jnp.zeros((32,), jnp.int32), holder[32:],
    ])

    def vmem(*shape):
        return pltpu.VMEM(shape, F32)

    def sems(n):
        return [pltpu.SemaphoreType.DMA((n,)), pltpu.SemaphoreType.DMA((n,))]

    smem = pl.BlockSpec(memory_space=pltpu.SMEM)
    whole = pl.BlockSpec(memory_space=pltpu.VMEM)
    charges = pl.pallas_call(
        kernel,
        out_shape=jax.ShapeDtypeStruct((2, LANES), F32),
        in_specs=[smem] * 4 + [whole] * 2,
        out_specs=whole,
        scratch_shapes=[
            vmem(NX, NZ, 2, 4, LANES), vmem(NQ, 2, 4, LANES), vmem(NQ, 2, 4, LANES),
            vmem(SLOTS, 4, LANES), vmem(SLOTS, 4, LANES), vmem(2, 4, LANES, LANES),
            vmem(2, PAIRS, LANES, LANES),
            vmem(SLOTS, 2, LANES), vmem(SLOTS, 2, LANES), vmem(SLOTS, 2, LANES),
            vmem(NX, NZ, 2, 4, LANES), vmem(NQ, 2, 4, LANES), vmem(NQ, 2, 4, LANES),
            vmem(2, 2, LANES), vmem(NZ, 2, LANES), vmem(NX, 2, LANES), vmem(NQ, 2, LANES), vmem(3, 2, LANES),
            *sems(NZ), *sems(NX), *sems(NQ), *sems(26), *sems(26), *sems(26),
            *sems(NZ), *sems(NX), *sems(NQ), *sems(NZ), *sems(NX), *sems(NQ),
        ],
        compiler_params=pltpu.CompilerParams(collective_id=0, has_side_effects=True),
    )(idx, chi_table, eta_table, gamma_table, offsets, types.reshape(2, LANES))
    return charges.reshape(2 * LANES)


def solution(mesh):
    torus = Mesh(mesh.devices.reshape(8, 2, 8, 4), AXES)
    placed = (P(None, AXES), P(), P(AXES), P(None, ("z", "x"), ("y", "c"), None), P(), P(), P())
    return jax.shard_map(
        per_device, mesh=torus, in_specs=placed, out_specs=P(AXES), check_vma=False
    )
```

```python
import jax
import jax.numpy as jnp
from jax import lax
from jax.experimental import pallas as pl
from jax.experimental.pallas import tpu as pltpu
from jax.sharding import Mesh
from jax.sharding import PartitionSpec as P

LANES = 128
NX, NY, NZ, NQ = 4, 8, 8, 16
OWN = 17
PAIRS = 27
SLOTS = 36
MOMENTS = 10
SHIFTS = (200.0, 20.0)
F32 = jnp.float32
AXES = ("y", "c", "z", "x")
BF16 = jnp.bfloat16
MESH = pl.DeviceIdType.MESH
KINDS = {"C1": (1, 1, 2), "CX": (2, 1, 4), "E1": (1, 2, 2), "EX": (2, 2, 4)}
TILES = {"C1": 4, "CX": 8, "E1": 2, "EX": 4}
CLASSES = [(p, k) for p in ("own", "sib", "far") for k in KINDS if (p, k) != ("own", "C1")]
ARRIVAL = [
    ("sib", "C1"), ("own", "CX"), ("own", "E1"), ("far", "C1"), ("sib", "CX"), ("sib", "E1"),
    ("own", "EX"), ("far", "CX"), ("far", "E1"), ("sib", "EX"), ("far", "EX"),
]


def far_first(n):
    return sorted(range(1, n), key=lambda k: -min(k, n - k))


def choose(kind, table):
    low = jnp.where(kind < 0.5, table[0], table[1])
    high = jnp.where(kind < 2.5, table[2], table[3])
    return jnp.where(kind < 1.5, low, high)


def await_bytes(ref, sem):
    pltpu.make_async_copy(ref, ref, sem).wait()


class Exchange:
    def __init__(self, peers, sems, whole):
        self.peers, self.sems, self.whole = peers, sems, whole

    def start(self, src, dst):
        for k, peer in self.peers:
            pltpu.make_async_remote_copy(
                src_ref=src(k), dst_ref=dst(k), send_sem=self.sems.at[0], recv_sem=self.sems.at[1],
                device_id=peer, device_id_type=MESH,
            ).start()

    def wait(self):
        await_bytes(self.whole, self.sems.at[1])

    def finish(self):
        await_bytes(self.whole, self.sems.at[0])


def kernel(
    chi_h, eta_h, gam_h, cells_h, off_h, typ_h, out,
    chi_t, eta_t, gam_t, cells_s, cells, off, typ,
    gat, sel, rcv, hal, tgt, hbuf, hv1, hv2, acc, accx,
    rgat, rsel, rrcv, own0, az, ax, aq, msgs,
    zs, xs, qs, hs, h1s, h2s, rzs, rxs, rqs, dzs, dxs, dqs, ls,
):
    my = lax.axis_index("y")
    mc = lax.axis_index("c")
    mz = lax.axis_index("z")
    mx = lax.axis_index("x")
    mq = my * 2 + mc
    col = mz * 4 + mx
    loads = [
        pltpu.make_async_copy(src, dst, ls.at[k])
        for k, (src, dst) in enumerate((
            (off_h, off), (typ_h, typ), (chi_h, chi_t), (cells_h, cells), (cells_h, cells_s), (eta_h, eta_t), (gam_h, gam_t),
        ))
    ]
    for load in loads:
        load.start()

    zpeers = [(k, {"z": lax.rem(mz + k, NZ)}) for k in far_first(NZ)]
    xpeers = [(k, {"x": lax.rem(mx + k, NX)}) for k in far_first(NX)]
    qpeers = []
    for k in sorted(range(1, NQ), key=lambda k: -min(k, NQ - k)):
        q = lax.rem(mq + k, NQ)
        qpeers.append((k, {"y": q // 2, "c": lax.rem(q, 2)}))
    zfar = lax.rem(mz + 2 * mc - 1 + NZ, NZ)
    place = {"own": (1, mc, mz), "sib": (2 - 2 * mc, 1 - mc, mz), "far": (2 * mc, 1 - mc, zfar)}
    landing = {"own": 1, "sib": 2 * mc, "far": 2 - 2 * mc}

    def neighbours(plane, kind):
        many_x, many_y, _ = KINDS[kind]
        _, pc, pz = place[plane]
        for ex in ((0,) if many_x == 1 else (-1, 1)):
            for ey in ((0,) if many_y == 1 else (-1, 1)):
                peer = {"z": pz, "c": pc, "x": lax.rem(mx + ex + NX, NX), "y": lax.rem(my + ey + NY, NY)}
                first, n = (0, 2) if ey == 0 else ((1, 1) if ey == 1 else (0, 1))
                slot = landing[plane] * 12 + (1 - ex) * 4 + first + 1 - 2 * ey
                yield peer, first, n, slot

    barrier = pltpu.get_barrier_semaphore()
    everyone = [peer for _, peer in zpeers + xpeers + qpeers]
    for cls in CLASSES:
        everyone += [n[0] for n in neighbours(*cls)]
    for peer in everyone:
        pl.semaphore_signal(barrier, inc=1, device_id=peer, device_id_type=MESH)

    loads[0].wait()
    loads[1].wait()
    for b in range(2):
        lanes = pl.ds(b * LANES, LANES)
        for comp in range(3):
            gat[mx, mz, b, comp : comp + 1, :] = off[comp : comp + 1, lanes]
        gat[mx, mz, b, 3:4, :] = typ[b : b + 1, :].astype(F32)
    pl.semaphore_wait(barrier, len(everyone))

    zg = Exchange(zpeers, zs, gat.at[0, pl.ds(0, NZ - 1)])
    zg.start(lambda k: gat.at[mx, mz], lambda k: gat.at[mx, mz])
    for load in loads[2:]:
        load.wait()
    lane = lax.broadcasted_iota(jnp.int32, (1, LANES), 1)
    near = pl.ds(pl.multiple_of((mq // 2) * LANES, LANES), LANES)
    mine = jnp.where(lane // 64 == lax.rem(mq, 2), (cells[0:1, near] * 16 + cells[1:2, near]) * 4 + cells[2:3, near], -1)

    def key_of(q, s):
        return ((2 * mz + lax.rem(q, 2)) * 16 + 2 * (q // 2) + s) * 4 + mx

    fwd = [jnp.max(jnp.where(mine == key_of(q, s), lax.rem(lane, 64), 0)) for q in range(NQ) for s in range(2)]
    owner = []
    every = (cells[0:1, :] * 16 + cells[1:2, :]) * 4 + cells[2:3, :]
    order = lax.broadcasted_iota(jnp.int32, every.shape, 1)
    for s in range(2):
        owner.append(jnp.max(jnp.where(every == key_of(mq, s), order // 64, 0)))
    for b in range(2):
        own0[b, 0:1, :] = -choose(gat[mx, mz, b, 3:4, :], chi_t)
        own0[b, 1:2, :] = jnp.full((1, LANES), -1.0, F32)
    zg.wait()
    xg = Exchange(xpeers, xs, gat.at[pl.ds(0, NX - 1)])
    xg.start(lambda k: gat.at[mx], lambda k: gat.at[mx])
    xg.wait()

    def pick_all(source, chosen, received, wanted):
        for q in range(NQ):
            for s in range(2):
                chosen[q, s] = source[wanted(q, s)]
        received[mq] = chosen[mq]

    def gathered(i):
        at = i // 2
        return lax.rem(at, 4), at // 4, lax.rem(i, 2)

    pick_all(gat, sel, rcv, lambda q, s: gathered(fwd[q * 2 + s]))
    qg = Exchange(qpeers, qs, sel.at[pl.ds(0, NQ - 1)])
    qg.start(lambda k: sel.at[lax.rem(mq + k, NQ)], lambda k: rcv.at[mq])
    qg.wait()
    for s in range(2):
        hal[OWN + s] = rcv[owner[s], s]

    def send_halo(ref, sems):
        for plane, kind in reversed(ARRIVAL):
            for peer, first, n, slot in neighbours(plane, kind):
                pltpu.make_async_remote_copy(
                    src_ref=ref.at[pl.ds(OWN + first, n)], dst_ref=ref.at[pl.ds(slot, n)],
                    send_sem=sems.at[len(CLASSES)], recv_sem=sems.at[CLASSES.index((plane, kind))],
                    device_id=peer, device_id_type=MESH,
                ).start()

    def wait_halo(ref, sems, cls):
        await_bytes(ref.at[pl.ds(0, KINDS[cls[1]][2])], sems.at[CLASSES.index(cls)])

    def sent_halo(ref, sems):
        await_bytes(ref.at[pl.ds(0, 34)], sems.at[len(CLASSES)])

    def tiles(cls, body):
        plane, kind = place[cls[0]][0], cls[1]

        def one(k, carry):
            if kind == "C1":
                t, gz, gy = k // 2, 1, 1 + lax.rem(k, 2)
            elif kind == "CX":
                t, gz, gy = lax.rem(k // 2, 2), 2 * (k // 4), 1 + lax.rem(k, 2)
            elif kind == "E1":
                t, gz, gy = k, 1, 3 * k
            else:
                t, gz, gy = lax.rem(k, 2), 2 * (k // 2), 3 * lax.rem(k, 2)
            body(t, plane, gz, gy)
            return carry
        lax.fori_loop(0, TILES[kind], one, 0)

    send_halo(hal, hs)

    def shield_of(kind):
        gam = choose(kind, gam_t)
        return (lax.rsqrt(gam) / gam) * (0.001 ** 0.5)

    rows = []
    for t in range(2):
        rows += [(hal[OWN + t, c : c + 1, :] + (11.0 * t if c == 1 else 0.0)) * 0.1 for c in range(3)]
        rows.append(shield_of(hal[OWN + t, 3:4, :]))
    turned = jnp.concatenate(rows, axis=0).T
    for t in range(2):
        for c in range(4):
            tgt[t, c] = jnp.broadcast_to(turned[:, t * 4 + c : t * 4 + c + 1], (LANES, LANES))
    acc[...] = jnp.zeros_like(acc)

    def build(t, plane, gz, gy, diagonal=False):
        slot = plane * 12 + gz * 4 + gy
        n = plane * 9 + gz * 3 + gy - t
        step = [plane - 1, gy - 1, gz - 1]
        src = [(hal[slot, c : c + 1, :] + jnp.asarray(step[c] * 11).astype(F32)) * 0.1 for c in range(3)]
        kind = hal[slot, 3:4, :]
        shield = shield_of(kind)
        chi = choose(kind, chi_t)
        eta = choose(kind, eta_t)
        for j in range(16):
            rows = pl.ds(j * 8, 8)
            dx = src[0] - tgt[t, 0, rows, :]
            dy = src[1] - tgt[t, 1, rows, :]
            dz = src[2] - tgt[t, 2, rows, :]
            r2 = jnp.maximum(dx * dx + dy * dy + dz * dz, 1e-30)
            r = r2 * lax.rsqrt(r2)
            cube = r2 * r + shield * tgt[t, 3, rows, :]
            inv = jnp.exp2(jnp.log2(cube) * (-1.0 / 3.0))
            u = jnp.maximum(1.0 - r, 0.0)
            u = u * u
            poly = ((28.8 * r + 14.4) * r + 5.76) * r + 1.44
            h = (u * u) * poly * inv
            if diagonal:
                away = lax.broadcasted_iota(jnp.int32, (8, LANES), 1) - lax.broadcasted_iota(jnp.int32, (8, LANES), 0)
                h = jnp.where(away == j * 8 + (gy - 1 - t) * 1024, eta, h)
            hbuf[t, n, rows, :] = h
            acc[t, 0, rows, :] += h * chi
            acc[t, 1, rows, :] += h

    tiles(("own", "C1"), lambda *at: build(*at, diagonal=True))
    for cls in ARRIVAL:
        wait_halo(hal, hs, cls)
        tiles(cls, build)

    ones = jnp.ones((8, LANES), BF16)

    def across(ref, t, rhs):
        whole = ref[t, rhs]
        high = whole.astype(BF16)
        low = (whole - high.astype(F32)).astype(BF16)
        dims = (((1,), (1,)), ((), ()))
        total = [lax.dot_general(ones, part, dims, preferred_element_type=F32) for part in (high, low)]
        return (total[0] + total[1])[0:1]

    def multiply(vec, ref):
        def one(t, plane, gz, gy):
            v = vec[plane * 12 + gz * 4 + gy]
            n = plane * 9 + gz * 3 + gy - t
            for j in range(16):
                rows = pl.ds(j * 8, 8)
                h = hbuf[t, n, rows, :]
                ref[t, 0, rows, :] += h * v[0:1, :]
                ref[t, 1, rows, :] += h * v[1:2, :]
        return one

    v0 = []
    for t in range(2):
        chi = choose(hal[OWN + t, 3:4, :], chi_t)
        v0.append(jnp.concatenate([-chi, jnp.full((1, LANES), -1.0, F32)], axis=0))
        hv1[OWN + t, 0:1, :] = SHIFTS[0] * chi - across(acc, t, 0)
        hv1[OWN + t, 1:2, :] = SHIFTS[0] - across(acc, t, 1)
    send_halo(hv1, h1s)
    accx[...] = jnp.zeros_like(accx)
    for e in (zg, xg, qg):
        e.finish()
    sent_halo(hal, hs)
    tiles(("own", "C1"), multiply(hv1, accx))
    for cls in ARRIVAL:
        wait_halo(hv1, h1s, cls)
        tiles(cls, multiply(hv1, accx))
    for t in range(2):
        for rhs in range(2):
            hv2[OWN + t, rhs : rhs + 1, :] = across(accx, t, rhs) - SHIFTS[1] * hv1[OWN + t, rhs : rhs + 1, :]
    send_halo(hv2, h2s)
    for t in range(2):
        rgat[mx, mz, t, 0:2, :] = hv1[OWN + t]
        rgat[mx, mz, t, 2:4, :] = hv2[OWN + t]
    rz = Exchange(zpeers, rzs, rgat.at[0, pl.ds(0, NZ - 1)])
    rz.start(lambda k: rgat.at[mx, mz], lambda k: rgat.at[mx, mz])
    acc[...] = jnp.zeros_like(acc)
    tiles(("own", "C1"), multiply(hv2, acc))

    lane2 = lax.broadcasted_iota(jnp.int32, (2, LANES), 1)
    v = [v0, [hv1[OWN + t] for t in range(2)], [hv2[OWN + t] for t in range(2)]]
    terms = [v[a][0] * v[b][0] + v[a][1] * v[b][1] for a, b in ((0, 0), (0, 1), (0, 2), (1, 1), (1, 2), (2, 2))]
    terms += [None] + [v[a][0] + v[a][1] for a in range(3)]
    msg = jnp.zeros((2, LANES), F32)
    for k, term in enumerate(terms):
        if term is not None:
            msg = jnp.where(lane2 == k, jnp.sum(term, axis=1, keepdims=True), msg)
    sent_halo(hv1, h1s)
    for cls in ARRIVAL:
        wait_halo(hv2, h2s, cls)
        tiles(cls, multiply(hv2, acc))
    image = [jnp.concatenate([across(acc, t, 0), across(acc, t, 1)], axis=0) for t in range(2)]
    term = v[2][0] * image[0] + v[2][1] * image[1]
    msg = jnp.where(lane2 == 6, jnp.sum(term, axis=1, keepdims=True), msg)
    msgs[0] = msg
    az[mz] = msg
    dz_ = Exchange(zpeers, dzs, az.at[pl.ds(0, NZ - 1)])
    dz_.start(lambda k: msgs.at[0], lambda k: az.at[mz])
    rz.wait()
    rx = Exchange(xpeers, rxs, rgat.at[pl.ds(0, NX - 1)])
    rx.start(lambda k: rgat.at[mx], lambda k: rgat.at[mx])
    sent_halo(hv2, h2s)
    rz.finish()

    def lies(b):
        cx, cy, cz = cells_s[0, b], cells_s[1, b], cells_s[2, b]
        return (cz, cx // 2, lax.rem(cy, 2)), (cy // 2) * 2 + lax.rem(cx, 2)

    back_at = [lies(q * 64 + col * 2 + s)[0] for q in range(NQ) for s in range(2)]
    holder = [lies(mq * 64 + col * 2 + s)[1] for s in range(2)]
    dz_.wait()
    msg = az[0]
    for k in range(1, NZ):
        msg = msg + az[k]
    msgs[1] = msg
    ax[mx] = msg
    dx_ = Exchange(xpeers, dxs, ax.at[pl.ds(0, NX - 1)])
    dx_.start(lambda k: msgs.at[1], lambda k: ax.at[mx])
    rx.wait()
    pick_all(rgat, rsel, rrcv, lambda q, s: back_at[q * 2 + s])
    rq = Exchange(qpeers, rqs, rsel.at[pl.ds(0, NQ - 1)])
    rq.start(lambda k: rsel.at[lax.rem(mq + k, NQ)], lambda k: rrcv.at[mq])
    dx_.wait()
    msg = ax[0]
    for k in range(1, NX):
        msg = msg + ax[k]
    msgs[2] = msg
    aq[mq] = msg
    dq_ = Exchange(qpeers, dqs, aq.at[pl.ds(0, NQ - 1)])
    dq_.start(lambda k: msgs.at[2], lambda k: aq.at[mq])
    for e in (rx, dz_, dx_):
        e.finish()
    rq.wait()
    rq.finish()
    back = [rrcv[holder[s], s] for s in range(2)]
    dq_.wait()
    msg = aq[0]
    for k in range(1, NQ):
        msg = msg + aq[k]

    m = [jnp.broadcast_to(msg[:, k : k + 1], (2, LANES)) for k in range(MOMENTS)]
    gram = {(0, 0): m[0], (0, 1): m[1], (0, 2): m[2], (1, 1): m[3], (1, 2): m[4], (2, 2): m[5]}
    sums = m[7:]

    def dot(i, j):
        return gram[min(i, j), max(i, j)]

    def image_dot(i, j):
        i, j = min(i, j), max(i, j)
        return m[6] if i == 2 else dot(i + 1, j) + SHIFTS[i] * dot(i, j)

    def quadratic(a, form):
        total = None
        for i, ai in enumerate(a):
            for j in range(i, len(a)):
                term = ai * a[j] * form(i, j)
                term = term if i == j else term + term
                total = term if total is None else total + term
        return total

    def image(a):
        res = [None] * (len(a) + 1)
        for i, ai in enumerate(a):
            res[i + 1] = ai
            res[i] = SHIFTS[i] * ai if res[i] is None else res[i] + SHIFTS[i] * ai
        return res

    def plus(a, scale, b):
        res = []
        for i in range(max(len(a), len(b))):
            ai = a[i] if i < len(a) else None
            bi = b[i] if i < len(b) else None
            if bi is None:
                res.append(ai)
            elif ai is None:
                res.append(scale * bi)
            else:
                res.append(ai + scale * bi)
        return res

    one = jnp.ones((2, LANES), F32)
    x, r, p = [], [one], [one]
    rr = m[0]
    for step in range(3):
        alpha = rr / quadratic(p, image_dot)
        x = plus(x, alpha, p)
        if step < 2:
            r = plus(r, -alpha, image(p))
            new = quadratic(r, dot)
            p = plus(r, new / rr, p)
            rr = new
    total = x[0] * sums[0] + x[1] * sums[1] + x[2] * sums[2]
    ratio = total[0:1] / total[1:2]
    for s in range(2):
        b = back[s]
        part = x[0] * own0[s] + x[1] * b[0:2] + x[2] * b[2:4]
        out[s : s + 1, :] = part[0:1] - ratio * part[1:2]
    dq_.finish()


def per_device(offsets, cells, types, mask, chi_table, eta_table, gamma_table):
    def vmem(*shape):
        return pltpu.VMEM(shape, F32)

    def sems(n=2):
        return pltpu.SemaphoreType.DMA((n,))

    table = pltpu.SMEM((4,), F32)
    charges = pl.pallas_call(
        kernel,
        out_shape=jax.ShapeDtypeStruct((2, LANES), F32),
        in_specs=[pl.BlockSpec(memory_space=pl.ANY)] * 6,
        out_specs=pl.BlockSpec(memory_space=pltpu.VMEM),
        scratch_shapes=[
            table, table, table, pltpu.SMEM(cells.shape, jnp.int32), pltpu.VMEM(cells.shape, jnp.int32),
            vmem(3, 2 * LANES), pltpu.VMEM((2, LANES), jnp.int32),
            vmem(NX, NZ, 2, 4, LANES), vmem(NQ, 2, 4, LANES), vmem(NQ, 2, 4, LANES),
            vmem(SLOTS, 4, LANES), vmem(2, 4, LANES, LANES), vmem(2, PAIRS, LANES, LANES),
            vmem(SLOTS, 2, LANES), vmem(SLOTS, 2, LANES), vmem(2, 2, LANES, LANES), vmem(2, 2, LANES, LANES),
            vmem(NX, NZ, 2, 4, LANES), vmem(NQ, 2, 4, LANES), vmem(NQ, 2, 4, LANES),
            vmem(2, 2, LANES), vmem(NZ, 2, LANES), vmem(NX, 2, LANES), vmem(NQ, 2, LANES), vmem(3, 2, LANES),
            *[sems()] * 3, *[sems(len(CLASSES) + 1)] * 3, *[sems()] * 6, sems(7),
        ],
        compiler_params=pltpu.CompilerParams(collective_id=0, has_side_effects=True),
    )(chi_table, eta_table, gamma_table, cells, offsets, types.reshape(2, LANES))
    return charges.reshape(2 * LANES)


def solution(mesh):
    torus = Mesh(mesh.devices.reshape(8, 2, 8, 4), AXES)
    placed = (P(None, AXES), P(), P(AXES), P(None, ("z", "x"), ("y", "c"), None), P(), P(), P())
    return jax.shard_map(
        per_device, mesh=torus, in_specs=placed, out_specs=P(AXES), check_vma=False
    )
```
